32 devices in a mesh: dp: 2 (over x), tp: 16 (over y, z, core).
Axes of the slice: x: 2, y: 2, z: 4, core: 2. Of those that a mesh axis runs over, the one named last changes fastest.
Arguments:
- x: bfloat16 [128, 2048], P('dp'), parts along dimension 0
- k_cache: bfloat16 [128, 4096, 16, 128], P('dp', None, 'tp'), parts along dimension 0
- v_cache: bfloat16 [128, 4096, 16, 128], P('dp', None, 'tp'), parts along dimension 0
- gain_a: bfloat16 [2048], replicated
- wq: bfloat16 [2048, 2048], P(None, 'tp')
- wo: bfloat16 [2048, 2048], P('tp')
- gain_m: bfloat16 [2048], replicated
- w_gate: bfloat16 [2048, 8192], P(None, 'tp')
- w_up: bfloat16 [2048, 8192], P(None, 'tp')
- w_down: bfloat16 [8192, 2048], P('tp')
Outputs:
- output: bfloat16 [128, 2048], P('dp'), parts along dimension 0
There are 2 independent parts. The reference program is written for one: setup_inputs(seed, part) draws one part's arguments, and reference() takes and returns one part's arrays. A program takes and returns all parts, laid end to end along the dimension named above; an argument that names none is the same for every part.
All inputs are finite; a program needn't handle non-finite values.
Results may differ from the reference program's by a relative error of at most 0.017.
Values are sent between devices in bfloat16 or wider.
A program may use at most 2 GiB of HBM per device.

```python
import jax
import jax.numpy as jnp
from jax import lax

BATCH = 64
CACHE = 4096
D = 2048
HEADS = 16
KV_HEADS = 16
HEAD = 128
FF = 8192
THETA = 10000


def setup_inputs(seed: int = 0, part: int = 0) -> dict:
    kx, kc, kw, kn, kq, ko, km, kg, ku, kd = jax.random.split(jax.random.key(seed), 10)
    kx, kc, kw = (jax.random.fold_in(k, part) for k in (kx, kc, kw))

    def weights(key, rows, columns):
        return jax.random.normal(key, (rows, columns), jnp.float32) * rows**-0.5

    drawn = {
        "x": jax.random.normal(kx, (BATCH, D), jnp.float32),
        "k_cache": 2 * jax.random.normal(kc, (BATCH, CACHE, KV_HEADS, HEAD), jnp.float32),
        "v_cache": 4 * jax.random.normal(kw, (BATCH, CACHE, KV_HEADS, HEAD), jnp.float32),
        "gain_a": 1 + 0.1 * jax.random.normal(kn, (D,), jnp.float32),
        "wq": 2 * weights(kq, D, HEADS * HEAD),
        "wo": weights(ko, HEADS * HEAD, D),
        "gain_m": 1 + 0.1 * jax.random.normal(km, (D,), jnp.float32),
        "w_gate": weights(kg, D, FF),
        "w_up": weights(ku, D, FF),
        "w_down": 2 * weights(kd, FF, D),
    }
    return {k: v.astype(jnp.bfloat16) for k, v in drawn.items()}


def normed(x, gain):
    wide = x.astype(jnp.float32)
    scale = lax.rsqrt(jnp.mean(wide * wide, -1, keepdims=True) + 1e-6)
    return (wide * scale * gain.astype(jnp.float32)).astype(jnp.bfloat16)


def turned(t, place, theta):
    half = t.shape[-1] // 2
    angle = place.astype(jnp.float32)[:, None] * theta ** (-jnp.arange(half, dtype=jnp.float32) / half)
    cos, sin = jnp.cos(angle)[:, None], jnp.sin(angle)[:, None]
    a, b = t[..., :half].astype(jnp.float32), t[..., half:].astype(jnp.float32)
    return jnp.concatenate([a * cos - b * sin, b * cos + a * sin], -1).astype(jnp.bfloat16)


def matmul(a, w):
    return jnp.dot(a, w, preferred_element_type=jnp.float32).astype(jnp.bfloat16)


def einsum(form, a, b):
    return jnp.einsum(form, a.astype(jnp.float32), b.astype(jnp.float32))


def seen_by(a, wq, k_cache, v_cache, head, theta):
    batch, cache, kv_heads = k_cache.shape[:3]
    place = jnp.full((batch,), cache - 1)
    q = turned(matmul(a, wq).reshape(batch, -1, head), place, theta).reshape(batch, kv_heads, -1, head)
    scores = einsum("bgsd,bugd->bgsu", q, k_cache) * head**-0.5
    weights = jax.nn.softmax(scores, -1).astype(jnp.bfloat16)
    return einsum("bgsu,bugd->bgsd", weights, v_cache).astype(jnp.bfloat16).reshape(batch, -1)


def hidden_of(b, w_gate, w_up):
    gate = jnp.dot(b, w_gate, preferred_element_type=jnp.float32)
    up = jnp.dot(b, w_up, preferred_element_type=jnp.float32)
    return (jax.nn.silu(gate) * up).astype(jnp.bfloat16)


def reference(x, k_cache, v_cache, gain_a, wq, wo, gain_m, w_gate, w_up, w_down):
    seen = seen_by(normed(x, gain_a), wq, k_cache, v_cache, HEAD, THETA)
    h = (x.astype(jnp.float32) + jnp.dot(seen, wo, preferred_element_type=jnp.float32)).astype(jnp.bfloat16)
    hidden = hidden_of(normed(h, gain_m), w_gate, w_up)
    return (h.astype(jnp.float32) + jnp.dot(hidden, w_down, preferred_element_type=jnp.float32)).astype(jnp.bfloat16)
```

```python
import functools

import jax
import jax.numpy as jnp
import numpy as np
from jax import lax
from jax.experimental import pallas as pl
from jax.experimental.pallas import tpu as pltpu
from jax.sharding import PartitionSpec as P

HEAD = 128
THETA = 10000
MESH = pl.DeviceIdType.MESH
LANES = 128
GROUP = 8
HALF = 4
DEPTH = 5
CHUNKS = ((0, 16), (16, 16), (32, 16), (48, 8), (56, 8))


def turns(place):
    half = HEAD // 2
    angle = place * float(THETA) ** (-np.arange(half, dtype=np.float64) / half)
    cos, sin = np.cos(angle), np.sin(angle)
    table = np.zeros((8, HEAD), np.float32)
    table[0] = np.concatenate([cos, cos])
    table[1] = np.concatenate([-sin, sin])
    return table


def kernel(n, x_hbm, ga_hbm, gm_hbm, cs_hbm, wq_hbm, wo_hbm, wg_hbm, wu_hbm, wd_hbm, k_hbm, v_hbm, y_hbm, *scratch):
    nc = len(CHUNKS)
    (x_v, ga_v, gm_v, cs_v, wq_v, wo_v, wg_v, wu_v, wd_v, kbuf, vbuf, q_s, attn_s), scratch = scratch[:13], scratch[13:]
    own1, send1, recv1, hall, own2, send2, recv2, ybuf = (scratch[i * nc : (i + 1) * nc] for i in range(8))
    in_sem, k_sem, v_sem, send_sem, recv_sem, out_sem = scratch[8 * nc :]
    batch, cache = k_hbm.shape[:2]
    groups = batch // GROUP
    steps = 2 * groups
    d = x_v.shape[1]
    me = lax.axis_index("tp")

    barrier = pltpu.get_barrier_semaphore()

    def greet(i, _):
        pl.semaphore_signal(barrier, inc=1, device_id={"tp": lax.rem(me + i, n)}, device_id_type=MESH)
        return _

    lax.fori_loop(1, n, greet, 0)

    def load(i, src, dst):
        return pltpu.make_async_copy(src, dst, in_sem.at[i])

    loads = [
        load(i, s, t)
        for i, (s, t) in enumerate(
            (
                (x_hbm, x_v),
                (wq_hbm, wq_v),
                (ga_hbm, ga_v),
                (cs_hbm, cs_v),
                (gm_hbm, gm_v),
                (wo_hbm, wo_v),
                (wg_hbm, wg_v),
                (wu_hbm, wu_v),
                (wd_hbm, wd_v),
            )
        )
    ]

    def k_copy(t):
        slot = lax.rem(t, DEPTH)
        return pltpu.make_async_copy(k_hbm.at[pl.ds(HALF * t, HALF)], kbuf.at[slot], k_sem.at[slot])

    def v_copy(t):
        slot = lax.rem(t, DEPTH)
        return pltpu.make_async_copy(v_hbm.at[pl.ds(HALF * t, HALF)], vbuf.at[slot], v_sem.at[slot])

    for i in range(5):
        loads[i].start()
    for t in range(DEPTH):
        k_copy(t).start()
        v_copy(t).start()
        if t == 1:
            loads[5].start()
        if t == 3:
            for i in (6, 7, 8):
                loads[i].start()

    def normed(blocks, gain_v):
        total = blocks[0] * blocks[0]
        for b in blocks[1:]:
            total = total + b * b
        scale = lax.rsqrt(jnp.sum(total, -1, keepdims=True) / d + 1e-6)
        gain = gain_v[...].astype(jnp.float32)
        return jnp.concatenate([(b * scale * gain[j : j + 1]).astype(jnp.bfloat16) for j, b in enumerate(blocks)], 1)

    for i in range(4):
        loads[i].wait()
    a = normed([x_v[:, j * LANES : (j + 1) * LANES].astype(jnp.float32) for j in range(d // LANES)], ga_v)
    q = jnp.dot(a, wq_v[...], preferred_element_type=jnp.float32).astype(jnp.bfloat16).astype(jnp.float32)
    q = q * cs_v[0:1] + pltpu.roll(q, HEAD // 2, 1) * cs_v[1:2]
    q_s[...] = q.reshape(groups, GROUP, HEAD)

    rows = lax.broadcasted_iota(jnp.int32, (GROUP, HEAD), 0)

    def half_step(g, h):
        t = 2 * g + h
        slot = lax.rem(t, DEPTH)
        tile = min(cache, 512)
        qg = q_s[g]
        q_wide = jnp.concatenate([jnp.where(rows == HALF * h + j, qg, 0.0) for j in range(HALF)], 1).astype(jnp.bfloat16)
        k_copy(t).wait()
        pieces = []
        for i in range(cache // tile):
            k = jnp.concatenate([kbuf[slot, j, i * tile : (i + 1) * tile, :] for j in range(HALF)], 1)
            pieces.append(lax.dot_general(q_wide, k, (((1,), (1,)), ((), ())), preferred_element_type=jnp.float32))
        s = jnp.concatenate(pieces, 1) * HEAD**-0.5

        @pl.when(t + DEPTH < steps)
        def _():
            k_copy(t + DEPTH).start()

        e = jnp.exp(s - jnp.max(s, -1, keepdims=True))
        w = (e * (1.0 / jnp.sum(e, -1, keepdims=True))).astype(jnp.bfloat16)
        v_copy(t).wait()
        out = None
        for i in range(cache // tile):
            v = jnp.concatenate([vbuf[slot, j, i * tile : (i + 1) * tile, :] for j in range(HALF)], 1)
            part = jnp.dot(w[:, i * tile : (i + 1) * tile], v, preferred_element_type=jnp.float32)
            out = part if out is None else out + part

        @pl.when(t + DEPTH < steps)
        def _():
            v_copy(t + DEPTH).start()

        return sum(jnp.where(rows == HALF * h + j, out[:, j * HEAD : (j + 1) * HEAD], 0.0) for j in range(HALF))

    def scatter(c, phase, send, recv):
        def body(i, _):
            j = lax.rem(me + i, n)
            pltpu.make_async_remote_copy(
                src_ref=send.at[j],
                dst_ref=recv.at[me],
                send_sem=send_sem.at[phase, c],
                recv_sem=recv_sem.at[phase, c],
                device_id={"tp": j},
                device_id_type=MESH,
            ).start()
            return _

        lax.fori_loop(1, n, body, 0)

    def wait(c, phase, sent, landed):
        copy = pltpu.make_async_remote_copy(
            src_ref=sent,
            dst_ref=landed,
            send_sem=send_sem.at[phase, c],
            recv_sem=recv_sem.at[phase, c],
            device_id={"tp": lax.rem(me + 1, n)},
            device_id_type=MESH,
        )
        return copy

    def put_term(c, term, own, send):
        for j in range(n):
            piece = term[:, j * LANES : (j + 1) * LANES]
            own[j] = piece
            send[j] = piece.astype(jnp.bfloat16)

    def total(own, recv):
        acc = own[me]
        for i in range(1, n):
            acc = acc + recv[lax.rem(me + i, n)].astype(jnp.float32)
        return acc

    def first(c):
        r0, r = CHUNKS[c]
        if c == 0:
            pl.semaphore_wait(barrier, n - 1)
            loads[5].wait()
        seen = jnp.concatenate([attn_s[i] for i in range(r0 // GROUP, (r0 + r) // GROUP)], 0).astype(jnp.bfloat16)
        put_term(c, jnp.dot(seen, wo_v[...], preferred_element_type=jnp.float32), own1[c], send1[c])
        scatter(c, 0, send1[c], recv1[c])

    def second(c):
        r0, r = CHUNKS[c]
        wait(c, 0, send1[c].at[pl.ds(0, n - 1)], recv1[c].at[pl.ds(0, n - 1)]).wait_recv()
        mine = x_v[r0 : r0 + r, pl.ds(pl.multiple_of(me * LANES, LANES), LANES)].astype(jnp.float32)
        hall[c][me] = (mine + total(own1[c], recv1[c])).astype(jnp.bfloat16)

        def body(i, _):
            pltpu.make_async_remote_copy(
                src_ref=hall[c].at[me],
                dst_ref=hall[c].at[me],
                send_sem=send_sem.at[1, c],
                recv_sem=recv_sem.at[1, c],
                device_id={"tp": lax.rem(me + i, n)},
                device_id_type=MESH,
            ).start()
            return _

        lax.fori_loop(1, n, body, 0)

    def third(c):
        wait(c, 1, hall[c].at[pl.ds(0, n - 1)], hall[c].at[pl.ds(0, n - 1)]).wait_recv()
        if c == 0:
            loads[4].wait()
            for i in (6, 7, 8):
                loads[i].wait()
        b = normed([hall[c][j].astype(jnp.float32) for j in range(n)], gm_v)
        gate = jnp.dot(b, wg_v[...], preferred_element_type=jnp.float32)
        up = jnp.dot(b, wu_v[...], preferred_element_type=jnp.float32)
        hidden = (jax.nn.silu(gate) * up).astype(jnp.bfloat16)
        put_term(c, jnp.dot(hidden, wd_v[...], preferred_element_type=jnp.float32), own2[c], send2[c])
        scatter(c, 2, send2[c], recv2[c])

    def fourth(c):
        r0, r = CHUNKS[c]
        wait(c, 2, send2[c].at[pl.ds(0, n - 1)], recv2[c].at[pl.ds(0, n - 1)]).wait_recv()
        ybuf[c][...] = (hall[c][me].astype(jnp.float32) + total(own2[c], recv2[c])).astype(jnp.bfloat16)
        block = y_hbm.at[pl.ds(r0, r), pl.ds(pl.multiple_of(me * LANES, LANES), LANES)]
        pltpu.make_async_copy(ybuf[c], block, out_sem.at[c]).start()

        def body(i, _):
            pltpu.make_async_remote_copy(
                src_ref=ybuf[c],
                dst_ref=block,
                send_sem=send_sem.at[3, c],
                recv_sem=recv_sem.at[3, c],
                device_id={"tp": lax.rem(me + i, n)},
                device_id_type=MESH,
            ).start()
            return _

        lax.fori_loop(1, n, body, 0)

    at = {
        1: [(first, 0)],
        2: [(second, 0)],
        3: [(third, 0), (first, 1)],
        4: [(fourth, 0), (second, 1)],
        5: [(third, 1), (first, 2)],
        6: [(fourth, 1), (second, 2), (first, 3)],
        7: [(third, 2), (second, 3), (first, 4)],
    }
    tail = [(third, 3), (fourth, 2), (second, 4), (fourth, 3), (third, 4), (fourth, 4)]

    def step(g, carry):
        attn_s[g] = half_step(g, 0) + half_step(g, 1)
        for when, work in at.items():

            @pl.when(g == when)
            def _():
                for stage, c in work:
                    stage(c)

        return carry

    lax.fori_loop(0, groups, step, 0)
    for stage, c in tail:
        stage(c)
    for c, (r0, r) in enumerate(CHUNKS):
        many = pl.ds(0, n - 1)
        wait(c, 0, send1[c].at[many], recv1[c].at[many]).wait_send()
        wait(c, 1, hall[c].at[many], hall[c].at[many]).wait_send()
        wait(c, 2, send2[c].at[many], recv2[c].at[many]).wait_send()
        block = y_hbm.at[pl.ds(r0, r), pl.ds(0, (n - 1) * LANES)]
        wait(c, 3, send2[c].at[many], block).wait_send()
        wait(c, 3, send2[c].at[many], block).wait_recv()
        pltpu.make_async_copy(ybuf[c], y_hbm.at[pl.ds(r0, r), pl.ds(0, LANES)], out_sem.at[c]).wait()


def solution(mesh):
    n = mesh.shape["tp"]

    def step(x, k_cache, v_cache, gain_a, wq, wo, gain_m, w_gate, w_up, w_down):
        batch, cache = k_cache.shape[:2]
        d, ff = x.shape[1], w_gate.shape[1]
        nc = len(CHUNKS)
        bf, f32 = jnp.bfloat16, jnp.float32
        per_chunk = []
        for dtype, lead in ((f32, True), (bf, True), (bf, True), (bf, True), (f32, True), (bf, True), (bf, True), (bf, False)):
            per_chunk += [pltpu.VMEM(((n,) if lead else ()) + (r, LANES), dtype) for _, r in CHUNKS]
        return pl.pallas_call(
            functools.partial(kernel, n),
            out_shape=jax.ShapeDtypeStruct(x.shape, x.dtype),
            in_specs=[pl.BlockSpec(memory_space=pl.ANY)] * 11,
            out_specs=pl.BlockSpec(memory_space=pl.ANY),
            scratch_shapes=[
                pltpu.VMEM(x.shape, bf),
                pltpu.VMEM((d // LANES, LANES), bf),
                pltpu.VMEM((d // LANES, LANES), bf),
                pltpu.VMEM((8, HEAD), f32),
                pltpu.VMEM(wq.shape, bf),
                pltpu.VMEM(wo.shape, bf),
                pltpu.VMEM(w_gate.shape, bf),
                pltpu.VMEM(w_up.shape, bf),
                pltpu.VMEM(w_down.shape, bf),
                pltpu.VMEM((DEPTH, HALF, cache, HEAD), bf),
                pltpu.VMEM((DEPTH, HALF, cache, HEAD), bf),
                pltpu.VMEM((batch // GROUP, GROUP, HEAD), f32),
                pltpu.VMEM((batch // GROUP, GROUP, HEAD), f32),
                *per_chunk,
                pltpu.SemaphoreType.DMA((9,)),
                pltpu.SemaphoreType.DMA((DEPTH,)),
                pltpu.SemaphoreType.DMA((DEPTH,)),
                pltpu.SemaphoreType.DMA((4, nc)),
                pltpu.SemaphoreType.DMA((4, nc)),
                pltpu.SemaphoreType.DMA((nc,)),
            ],
            compiler_params=pltpu.CompilerParams(
                collective_id=0, has_side_effects=True, vmem_limit_bytes=66 * 1024 * 1000
            ),
        )(
            x,
            gain_a.reshape(d // LANES, LANES),
            gain_m.reshape(d // LANES, LANES),
            jnp.asarray(turns(cache - 1)),
            wq,
            wo,
            w_gate,
            w_up,
            w_down,
            k_cache.reshape(batch, cache, HEAD),
            v_cache.reshape(batch, cache, HEAD),
        )

    states, cache, columns, rows_of = P("dp", None), P("dp", None, "tp", None), P(None, "tp"), P("tp", None)
    return jax.shard_map(
        step,
        mesh=mesh,
        in_specs=(states, cache, cache, P(None), columns, rows_of, P(None), columns, columns, rows_of),
        out_specs=states,
        check_vma=False,
    )
```

```python
import functools

import jax
import jax.numpy as jnp
import numpy as np
from jax import lax
from jax.experimental import pallas as pl
from jax.experimental.pallas import tpu as pltpu
from jax.sharding import PartitionSpec as P

HEAD = 128
THETA = 10000
MESH = pl.DeviceIdType.MESH
LANES = 128
GROUP = 8
HALF = 4
DEPTH = 4
CHUNKS = ((0, 24), (24, 16), (40, 16), (56, 8))
OWNERS = ((2, 4, 10, 12), (2, 4, 10, 12), (2, 4, 10, 12), (3, 5, 11, 13))


def turns(place):
    half = HEAD // 2
    angle = place * float(THETA) ** (-np.arange(half, dtype=np.float64) / half)
    cos, sin = np.cos(angle), np.sin(angle)
    table = np.zeros((8, HEAD), np.float32)
    table[0] = np.concatenate([cos, cos])
    table[1] = np.concatenate([-sin, sin])
    return table


def kernel(n, x_hbm, ga_hbm, gm_hbm, cs_hbm, wq_hbm, wo_hbm, wg_hbm, wu_hbm, wd_hbm, k_hbm, v_hbm, y_v, *scratch):
    nc = len(CHUNKS)
    (x_v, ga_v, gm_v, cs_v, wq_v, wo_v, wg_v, wu_v, wd_v, kbuf, vbuf, q_s, attn_s, w_s), scratch = scratch[:14], scratch[14:]
    own1, send1, recv1, hall, own2, send2, recv2, ybuf = (scratch[i * nc : (i + 1) * nc] for i in range(8))
    in_sem, k_sem, v_sem, send_sem, recv_sem = scratch[8 * nc :]
    batch, cache = k_hbm.shape[:2]
    groups = batch // GROUP
    steps = 2 * groups
    d = x_v.shape[1]
    me = lax.axis_index("tp")

    barrier = pltpu.get_barrier_semaphore()

    def load(i, src, dst):
        return pltpu.make_async_copy(src, dst, in_sem.at[i])

    loads = [
        load(i, s, t)
        for i, (s, t) in enumerate(
            (
                (x_hbm, x_v),
                (wq_hbm, wq_v),
                (ga_hbm, ga_v),
                (cs_hbm, cs_v),
                (gm_hbm, gm_v),
                (wo_hbm, wo_v),
                (wg_hbm, wg_v),
                (wu_hbm, wu_v),
                (wd_hbm, wd_v),
            )
        )
    ]

    def k_copy(t):
        slot = lax.rem(t, DEPTH)
        return pltpu.make_async_copy(k_hbm.at[pl.ds(HALF * t, HALF)], kbuf.at[slot], k_sem.at[slot])

    def v_copy(t):
        slot = lax.rem(t, DEPTH)
        return pltpu.make_async_copy(v_hbm.at[pl.ds(HALF * t, HALF)], vbuf.at[slot], v_sem.at[slot])

    for i in range(5):
        loads[i].start()
    for t in range(DEPTH):
        k_copy(t).start()
        v_copy(t).start()
        if t == 1:
            loads[5].start()
        if t == 3:
            for i in (6, 7, 8):
                loads[i].start()

    def greet(i, _):
        pl.semaphore_signal(barrier, inc=1, device_id={"tp": lax.rem(me + i, n)}, device_id_type=MESH)
        return _

    lax.fori_loop(1, n, greet, 0)

    def normed(blocks, gain_v):
        total = blocks[0] * blocks[0]
        for b in blocks[1:]:
            total = total + b * b
        scale = lax.rsqrt(jnp.sum(total, -1, keepdims=True) / d + 1e-6)
        gain = gain_v[...].astype(jnp.float32)
        return jnp.concatenate([(b * scale * gain[j : j + 1]).astype(jnp.bfloat16) for j, b in enumerate(blocks)], 1)

    for i in range(4):
        loads[i].wait()
    a = normed([x_v[:, j * LANES : (j + 1) * LANES].astype(jnp.float32) for j in range(d // LANES)], ga_v)
    q = jnp.dot(a, wq_v[...], preferred_element_type=jnp.float32).astype(jnp.bfloat16).astype(jnp.float32)
    q = q * cs_v[0:1] + pltpu.roll(q, HEAD // 2, 1) * cs_v[1:2]
    q_s[...] = q.reshape(groups, GROUP, HEAD)

    rows = lax.broadcasted_iota(jnp.int32, (GROUP, HEAD), 0)

    tile = min(cache, 512)

    def score(g, h):
        t = 2 * g + h
        slot = lax.rem(t, DEPTH)
        qg = q_s[g]
        q_wide = jnp.concatenate([jnp.where(rows == HALF * h + j, qg, 0.0) for j in range(HALF)], 1).astype(jnp.bfloat16)
        pieces = []
        for i in range(cache // tile):
            k = jnp.concatenate([kbuf[slot, j, i * tile : (i + 1) * tile, :] for j in range(HALF)], 1)
            pieces.append(lax.dot_general(q_wide, k, (((1,), (1,)), ((), ())), preferred_element_type=jnp.float32))
        s = jnp.concatenate(pieces, 1) * HEAD**-0.5
        e = jnp.exp(s - jnp.max(s, -1, keepdims=True))
        w_s[h] = (e * (1.0 / jnp.sum(e, -1, keepdims=True))).astype(jnp.bfloat16)

    def weigh(g, h):
        slot = lax.rem(2 * g + h, DEPTH)
        out = None
        for i in range(cache // tile):
            v = jnp.concatenate([vbuf[slot, j, i * tile : (i + 1) * tile, :] for j in range(HALF)], 1)
            part = jnp.dot(w_s[h, :, i * tile : (i + 1) * tile], v, preferred_element_type=jnp.float32)
            out = part if out is None else out + part
        return sum(jnp.where(rows == HALF * h + j, out[:, j * HEAD : (j + 1) * HEAD], 0.0) for j in range(HALF))

    def refill(copy, t):
        @pl.when(t + DEPTH < steps)
        def _():
            copy(t + DEPTH).start()

    my_y, my_z = me // 8, lax.rem(me, 8) // 2

    def place(c):
        mine = jnp.logical_and(lax.rem(me, 2) == OWNERS[c][0] % 2, jnp.logical_or(my_z == 1, my_z == 2))
        return mine, 2 * my_y + jnp.where(my_z == 2, 1, 0)

    def send(c, phase, src, dst, j):
        pltpu.make_async_remote_copy(
            src_ref=src,
            dst_ref=dst,
            send_sem=send_sem.at[phase, c],
            recv_sem=recv_sem.at[phase, c],
            device_id={"tp": j},
            device_id_type=MESH,
        ).start()

    def scatter(c, phase, src, dst):
        far = jnp.where(my_z < 2, 2, 1)
        for z in (far, 3 - far):
            for y in (1 - my_y, my_y):
                o = 8 * y + 2 * z + OWNERS[c][0] % 2

                @pl.when(me != o)
                def _():
                    send(c, phase, src.at[2 * y + z - 1], dst.at[me], o)

    def spread(c, phase, src, dst):
        core = OWNERS[c][0] % 2
        for z in (3, 2, 0, 1):
            for y in (1 - my_y, my_y):
                for other in (1 - core, core):
                    if z != 1 or y is not my_y or other != core:
                        send(c, phase, src, dst, 8 * y + 2 * (z + (my_z - 1) * (3 - 2 * z)) + other)

    def waits(c, phase, ref):
        return pltpu.make_async_remote_copy(
            src_ref=ref,
            dst_ref=ref,
            send_sem=send_sem.at[phase, c],
            recv_sem=recv_sem.at[phase, c],
            device_id={"tp": lax.rem(me + 1, n)},
            device_id_type=MESH,
        )

    def wait_pieces(c, phase, ref, sent=False):
        mine, _ = place(c)
        many = len(OWNERS[c])

        def wait(k):
            copy = waits(c, phase, ref.at[pl.ds(0, k)])
            copy.wait_send() if sent else copy.wait_recv()

        @pl.when(mine)
        def _():
            wait(many - 1)

        @pl.when(jnp.logical_not(mine))
        def _():
            wait(many)

    def put_term(c, term, own, out):
        w = d // len(OWNERS[c])
        for p in range(len(OWNERS[c])):
            piece = term[:, p * w : (p + 1) * w]
            own[p] = piece
            out[p] = piece.astype(jnp.bfloat16)

    def total(piece, own, recv):
        acc = own[piece]
        for i in range(1, n):
            acc = acc + recv[lax.rem(me + i, n)].astype(jnp.float32)
        return acc

    def first(c):
        r0, r = CHUNKS[c]
        if c == 0:
            pl.semaphore_wait(barrier, n - 1)
            loads[5].wait()
        seen = jnp.concatenate([attn_s[i] for i in range(r0 // GROUP, (r0 + r) // GROUP)], 0).astype(jnp.bfloat16)
        put_term(c, jnp.dot(seen, wo_v[...], preferred_element_type=jnp.float32), own1[c], send1[c])
        scatter(c, 0, send1[c], recv1[c])

    def second(c):
        r0, r = CHUNKS[c]
        w = d // len(OWNERS[c])
        mine, piece = place(c)

        @pl.when(mine)
        def _():
            waits(c, 0, recv1[c].at[pl.ds(0, n - 1)]).wait_recv()
            x = x_v[r0 : r0 + r, pl.ds(pl.multiple_of(piece * w, w), w)].astype(jnp.float32)
            hall[c][piece] = (x + total(piece, own1[c], recv1[c])).astype(jnp.bfloat16)
            spread(c, 1, hall[c].at[piece], hall[c].at[piece])

    def third(c):
        many = len(OWNERS[c])
        w = d // many
        wait_pieces(c, 1, hall[c])
        if c == 0:
            loads[4].wait()
            for i in (6, 7, 8):
                loads[i].wait()
        blocks = [
            hall[c][p, :, i * LANES : (i + 1) * LANES].astype(jnp.float32) for p in range(many) for i in range(w // LANES)
        ]
        b = normed(blocks, gm_v)
        gate = jnp.dot(b, wg_v[...], preferred_element_type=jnp.float32)
        up = jnp.dot(b, wu_v[...], preferred_element_type=jnp.float32)
        hidden = (jax.nn.silu(gate) * up).astype(jnp.bfloat16)
        put_term(c, jnp.dot(hidden, wd_v[...], preferred_element_type=jnp.float32), own2[c], send2[c])
        scatter(c, 2, send2[c], recv2[c])

    def block_of(c, piece):
        r0, r = CHUNKS[c]
        w = d // len(OWNERS[c])
        return y_v.at[pl.ds(r0, r), pl.ds(pl.multiple_of(piece * w, w), w)]

    def fourth(c):
        mine, piece = place(c)

        @pl.when(mine)
        def _():
            waits(c, 2, recv2[c].at[pl.ds(0, n - 1)]).wait_recv()
            ybuf[c][...] = (hall[c][piece].astype(jnp.float32) + total(piece, own2[c], recv2[c])).astype(jnp.bfloat16)
            spread(c, 3, ybuf[c], block_of(c, piece))
            block_of(c, piece)[...] = ybuf[c][...]

    at = {
        2: [(first, 0)],
        3: [(second, 0)],
        4: [(first, 1), (third, 0)],
        5: [(second, 1), (fourth, 0)],
        6: [(first, 2), (third, 1)],
    }
    tail = [(first, 3), (second, 2), (fourth, 1), (second, 3), (third, 2), (third, 3), (fourth, 2), (fourth, 3)]

    def second_half(g):
        k_copy(2 * g + 1).wait()
        v_copy(2 * g).wait()
        score(g, 1)
        attn_s[g] = weigh(g, 0)
        refill(k_copy, 2 * g + 1)
        refill(v_copy, 2 * g)

    def step(g, carry):
        second_half(g)
        k_copy(2 * g + 2).wait()
        v_copy(2 * g + 1).wait()
        score(g + 1, 0)
        attn_s[g] = attn_s[g] + weigh(g, 1)
        refill(k_copy, 2 * g + 2)
        refill(v_copy, 2 * g + 1)
        for when, work in at.items():

            @pl.when(g == when)
            def _():
                for stage, c in work:
                    stage(c)

        return carry

    k_copy(0).wait()
    score(0, 0)
    refill(k_copy, 0)
    lax.fori_loop(0, groups - 1, step, 0)
    second_half(groups - 1)
    v_copy(steps - 1).wait()
    attn_s[groups - 1] = attn_s[groups - 1] + weigh(groups - 1, 1)
    for stage, c in tail:
        stage(c)
    for c in range(nc):
        mine, _ = place(c)
        wait_pieces(c, 0, send1[c], True)
        wait_pieces(c, 2, send2[c], True)

        @pl.when(mine)
        def _():
            waits(c, 1, recv1[c].at[pl.ds(0, n - 1)]).wait_send()
            waits(c, 3, recv1[c].at[pl.ds(0, n - 1)]).wait_send()

        wait_pieces(c, 3, send1[c])


def solution(mesh):
    n = mesh.shape["tp"]

    def step(x, k_cache, v_cache, gain_a, wq, wo, gain_m, w_gate, w_up, w_down):
        batch, cache = k_cache.shape[:2]
        d, ff = x.shape[1], w_gate.shape[1]
        nc = len(CHUNKS)
        bf, f32 = jnp.bfloat16, jnp.float32
        sizes = [(len(o), r, d // len(o)) for o, (_, r) in zip(OWNERS, CHUNKS)]
        per_chunk = []
        for half in range(2):
            per_chunk += [pltpu.VMEM((k, r, w), f32) for k, r, w in sizes]
            per_chunk += [pltpu.VMEM((k, r, w), bf) for k, r, w in sizes]
            per_chunk += [pltpu.VMEM((n, r, w), bf) for _, r, w in sizes]
            per_chunk += [pltpu.VMEM((r, w) if half else (k, r, w), bf) for k, r, w in sizes]
        return pl.pallas_call(
            functools.partial(kernel, n),
            out_shape=pltpu.VMEM(x.shape, x.dtype),
            in_specs=[pl.BlockSpec(memory_space=pltpu.HBM)] * 11,
            out_specs=pl.BlockSpec(memory_space=pltpu.VMEM),
            scratch_shapes=[
                pltpu.VMEM(x.shape, bf),
                pltpu.VMEM((d // LANES, LANES), bf),
                pltpu.VMEM((d // LANES, LANES), bf),
                pltpu.VMEM((8, HEAD), f32),
                pltpu.VMEM(wq.shape, bf),
                pltpu.VMEM(wo.shape, bf),
                pltpu.VMEM(w_gate.shape, bf),
                pltpu.VMEM(w_up.shape, bf),
                pltpu.VMEM(w_down.shape, bf),
                pltpu.VMEM((DEPTH, HALF, cache, HEAD), bf),
                pltpu.VMEM((DEPTH, HALF, cache, HEAD), bf),
                pltpu.VMEM((batch // GROUP, GROUP, HEAD), f32),
                pltpu.VMEM((batch // GROUP, GROUP, HEAD), f32),
                pltpu.VMEM((2, GROUP, cache), bf),
                *per_chunk,
                pltpu.SemaphoreType.DMA((9,)),
                pltpu.SemaphoreType.DMA((DEPTH,)),
                pltpu.SemaphoreType.DMA((DEPTH,)),
                pltpu.SemaphoreType.DMA((4, nc)),
                pltpu.SemaphoreType.DMA((4, nc)),
            ],
            compiler_params=pltpu.CompilerParams(
                collective_id=0, has_side_effects=True, vmem_limit_bytes=56 * 1024 * 1024
            ),
        )(
            x,
            gain_a.reshape(d // LANES, LANES),
            gain_m.reshape(d // LANES, LANES),
            jnp.asarray(turns(cache - 1)),
            wq,
            wo,
            w_gate,
            w_up,
            w_down,
            k_cache.reshape(batch, cache, HEAD),
            v_cache.reshape(batch, cache, HEAD),
        )

    states, cache, columns, rows_of = P("dp", None), P("dp", None, "tp", None), P(None, "tp"), P("tp", None)
    return jax.shard_map(
        step,
        mesh=mesh,
        in_specs=(states, cache, cache, P(None), columns, rows_of, P(None), columns, columns, rows_of),
        out_specs=states,
        check_vma=False,
    )
```

```python
import functools

import jax
import jax.numpy as jnp
import numpy as np
from jax import lax
from jax.experimental import pallas as pl
from jax.experimental.pallas import tpu as pltpu
from jax.sharding import PartitionSpec as P

HEAD = 128
THETA = 10000
MESH = pl.DeviceIdType.MESH
LANES = 128
GROUP = 8
HALF = 4
DEPTH = 4
CHUNKS = ((0, 24), (24, 16), (40, 16), (56, 8))
OWNERS = ((3, 5, 11, 13), (3, 5, 11, 13), (3, 5, 11, 13), (3, 5, 11, 13))


def turns(place):
    half = HEAD // 2
    angle = place * float(THETA) ** (-np.arange(half, dtype=np.float64) / half)
    cos, sin = np.cos(angle), np.sin(angle)
    table = np.zeros((8, HEAD), np.float32)
    table[0] = np.concatenate([cos, cos])
    table[1] = np.concatenate([-sin, sin])
    return table


def kernel(n, x_hbm, ga_hbm, gm_hbm, cs_hbm, wq_hbm, wo_hbm, wg_hbm, wu_hbm, wd_hbm, k_hbm, v_hbm, y_v, *scratch):
    nc = len(CHUNKS)
    (x_v, ga_v, gm_v, cs_v, wq_v, wo_v, wg_v, wu_v, wd_v, kbuf, vbuf, q_s, attn_s, w_s), scratch = scratch[:14], scratch[14:]
    own1, send1, recv1, hall, own2, send2, recv2, ybuf = (scratch[i * nc : (i + 1) * nc] for i in range(8))
    in_sem, k_sem, v_sem, send_sem, recv_sem = scratch[8 * nc :]
    batch, cache = k_hbm.shape[:2]
    groups = batch // GROUP
    steps = 2 * groups
    d = x_v.shape[1]
    me = lax.axis_index("tp")

    barrier = pltpu.get_barrier_semaphore()

    def load(i, src, dst):
        return pltpu.make_async_copy(src, dst, in_sem.at[i])

    loads = [
        load(i, s, t)
        for i, (s, t) in enumerate(
            (
                (x_hbm, x_v),
                (wq_hbm, wq_v),
                (ga_hbm, ga_v),
                (cs_hbm, cs_v),
                (gm_hbm, gm_v),
                (wo_hbm, wo_v),
                (wg_hbm, wg_v),
                (wu_hbm, wu_v),
                (wd_hbm, wd_v),
            )
        )
    ]

    def k_copy(t):
        slot = lax.rem(t, DEPTH)
        return pltpu.make_async_copy(k_hbm.at[pl.ds(HALF * t, HALF)], kbuf.at[slot], k_sem.at[slot])

    def v_copy(t):
        slot = lax.rem(t, DEPTH)
        return pltpu.make_async_copy(v_hbm.at[pl.ds(HALF * t, HALF)], vbuf.at[slot], v_sem.at[slot])

    for i in range(5):
        loads[i].start()
    for t in range(DEPTH):
        k_copy(t).start()
        v_copy(t).start()
        if t == 1:
            loads[5].start()
        if t == 3:
            for i in (6, 7, 8):
                loads[i].start()

    def greet(i, _):
        pl.semaphore_signal(barrier, inc=1, device_id={"tp": lax.rem(me + i, n)}, device_id_type=MESH)
        return _

    lax.fori_loop(1, n, greet, 0)

    def normed(blocks, gain_v):
        total = blocks[0] * blocks[0]
        for b in blocks[1:]:
            total = total + b * b
        scale = lax.rsqrt(jnp.sum(total, -1, keepdims=True) / d + 1e-6)
        gain = gain_v[...].astype(jnp.float32)
        return jnp.concatenate([(b * scale * gain[j : j + 1]).astype(jnp.bfloat16) for j, b in enumerate(blocks)], 1)

    for i in range(4):
        loads[i].wait()
    a = normed([x_v[:, j * LANES : (j + 1) * LANES].astype(jnp.float32) for j in range(d // LANES)], ga_v)
    q = jnp.dot(a, wq_v[...], preferred_element_type=jnp.float32).astype(jnp.bfloat16).astype(jnp.float32)
    q = q * cs_v[0:1] + pltpu.roll(q, HEAD // 2, 1) * cs_v[1:2]
    q_s[...] = q.reshape(groups, GROUP, HEAD)

    rows = lax.broadcasted_iota(jnp.int32, (GROUP, HEAD), 0)

    tile = min(cache, 512)

    def score(g, h):
        t = 2 * g + h
        slot = lax.rem(t, DEPTH)
        qg = q_s[g]
        q_wide = jnp.concatenate([jnp.where(rows == HALF * h + j, qg, 0.0) for j in range(HALF)], 1).astype(jnp.bfloat16)
        pieces = []
        for i in range(cache // tile):
            k = jnp.concatenate([kbuf[slot, j, i * tile : (i + 1) * tile, :] for j in range(HALF)], 1)
            pieces.append(lax.dot_general(q_wide, k, (((1,), (1,)), ((), ())), preferred_element_type=jnp.float32))
        s = jnp.concatenate(pieces, 1) * HEAD**-0.5
        e = jnp.exp(s - jnp.max(s, -1, keepdims=True))
        w_s[h] = (e * (1.0 / jnp.sum(e, -1, keepdims=True))).astype(jnp.bfloat16)

    def weigh(g, h):
        slot = lax.rem(2 * g + h, DEPTH)
        out = None
        for i in range(cache // tile):
            v = jnp.concatenate([vbuf[slot, j, i * tile : (i + 1) * tile, :] for j in range(HALF)], 1)
            part = jnp.dot(w_s[h, :, i * tile : (i + 1) * tile], v, preferred_element_type=jnp.float32)
            out = part if out is None else out + part
        return sum(jnp.where(rows == HALF * h + j, out[:, j * HEAD : (j + 1) * HEAD], 0.0) for j in range(HALF))

    def refill(copy, t):
        @pl.when(t + DEPTH < steps)
        def _():
            copy(t + DEPTH).start()

    my_y, my_z = me // 8, lax.rem(me, 8) // 2

    def place(c):
        mine = jnp.logical_and(lax.rem(me, 2) == OWNERS[c][0] % 2, jnp.logical_or(my_z == 1, my_z == 2))
        return mine, 2 * my_y + jnp.where(my_z == 2, 1, 0)

    def send(c, phase, src, dst, j):
        pltpu.make_async_remote_copy(
            src_ref=src,
            dst_ref=dst,
            send_sem=send_sem.at[phase, c],
            recv_sem=recv_sem.at[phase, c],
            device_id={"tp": j},
            device_id_type=MESH,
        ).start()

    def scatter(c, phase, src, dst):
        far = jnp.where(my_z < 2, 2, 1)
        for z in (far, 3 - far):
            for y in (1 - my_y, my_y):
                o = 8 * y + 2 * z + OWNERS[c][0] % 2

                @pl.when(me != o)
                def _():
                    send(c, phase, src.at[2 * y + z - 1], dst.at[me], o)

    def spread(c, phase, src, dst):
        core = OWNERS[c][0] % 2
        for z in (3, 2, 0, 1):
            for y in (1 - my_y, my_y):
                for other in (1 - core, core):
                    if z != 1 or y is not my_y or other != core:
                        send(c, phase, src, dst, 8 * y + 2 * (z + (my_z - 1) * (3 - 2 * z)) + other)

    def waits(c, phase, ref):
        return pltpu.make_async_remote_copy(
            src_ref=ref,
            dst_ref=ref,
            send_sem=send_sem.at[phase, c],
            recv_sem=recv_sem.at[phase, c],
            device_id={"tp": lax.rem(me + 1, n)},
            device_id_type=MESH,
        )

    def wait_pieces(c, phase, ref, sent=False):
        mine, _ = place(c)
        many = len(OWNERS[c])

        def wait(k):
            copy = waits(c, phase, ref.at[pl.ds(0, k)])
            copy.wait_send() if sent else copy.wait_recv()

        @pl.when(mine)
        def _():
            wait(many - 1)

        @pl.when(jnp.logical_not(mine))
        def _():
            wait(many)

    def put_term(c, term, own, out):
        w = d // len(OWNERS[c])
        for p in range(len(OWNERS[c])):
            piece = term[:, p * w : (p + 1) * w]
            own[p] = piece
            out[p] = piece.astype(jnp.bfloat16)

    def total(piece, own, recv):
        acc = own[piece]
        for i in range(1, n):
            acc = acc + recv[lax.rem(me + i, n)].astype(jnp.float32)
        return acc

    def first(c):
        r0, r = CHUNKS[c]
        if c == 0:
            pl.semaphore_wait(barrier, n - 1)
            loads[5].wait()
        seen = jnp.concatenate([attn_s[i] for i in range(r0 // GROUP, (r0 + r) // GROUP)], 0).astype(jnp.bfloat16)
        put_term(c, jnp.dot(seen, wo_v[...], preferred_element_type=jnp.float32), own1[c], send1[c])
        scatter(c, 0, send1[c], recv1[c])

    def second(c):
        r0, r = CHUNKS[c]
        w = d // len(OWNERS[c])
        mine, piece = place(c)

        @pl.when(mine)
        def _():
            waits(c, 0, recv1[c].at[pl.ds(0, n - 1)]).wait_recv()
            x = x_v[r0 : r0 + r, pl.ds(pl.multiple_of(piece * w, w), w)].astype(jnp.float32)
            hall[c][piece] = (x + total(piece, own1[c], recv1[c])).astype(jnp.bfloat16)
            spread(c, 1, hall[c].at[piece], hall[c].at[piece])

    def third(c):
        many = len(OWNERS[c])
        w = d // many
        wait_pieces(c, 1, hall[c])
        if c == 0:
            loads[4].wait()
            for i in (6, 7, 8):
                loads[i].wait()
        blocks = [
            hall[c][p, :, i * LANES : (i + 1) * LANES].astype(jnp.float32) for p in range(many) for i in range(w // LANES)
        ]
        b = normed(blocks, gm_v)
        half = wg_v.shape[1] // 2
        term = None
        for i in range(2):
            gate = jnp.dot(b, wg_v[:, i * half : (i + 1) * half], preferred_element_type=jnp.float32)
            up = jnp.dot(b, wu_v[:, i * half : (i + 1) * half], preferred_element_type=jnp.float32)
            hidden = (jax.nn.silu(gate) * up).astype(jnp.bfloat16)
            part = jnp.dot(hidden, wd_v[i * half : (i + 1) * half, :], preferred_element_type=jnp.float32)
            term = part if term is None else term + part
        put_term(c, term, own2[c], send2[c])
        scatter(c, 2, send2[c], recv2[c])

    def block_of(c, piece):
        r0, r = CHUNKS[c]
        w = d // len(OWNERS[c])
        return y_v.at[pl.ds(r0, r), pl.ds(pl.multiple_of(piece * w, w), w)]

    def fourth(c):
        mine, piece = place(c)

        @pl.when(mine)
        def _():
            waits(c, 2, recv2[c].at[pl.ds(0, n - 1)]).wait_recv()
            ybuf[c][...] = (hall[c][piece].astype(jnp.float32) + total(piece, own2[c], recv2[c])).astype(jnp.bfloat16)
            spread(c, 3, ybuf[c], block_of(c, piece))
            block_of(c, piece)[...] = ybuf[c][...]

    at = {
        2: [(first, 0)],
        3: [(second, 0)],
        4: [(first, 1), (third, 0)],
        5: [(second, 1), (fourth, 0)],
        6: [(first, 2)],
    }
    tail = [(first, 3), (second, 2), (third, 1), (second, 3), (third, 2), (fourth, 1), (third, 3), (fourth, 2), (fourth, 3)]

    def second_half(g):
        k_copy(2 * g + 1).wait()
        v_copy(2 * g).wait()
        score(g, 1)
        attn_s[g] = weigh(g, 0)
        refill(k_copy, 2 * g + 1)
        refill(v_copy, 2 * g)

    def step(g, carry):
        second_half(g)
        k_copy(2 * g + 2).wait()
        v_copy(2 * g + 1).wait()
        score(g + 1, 0)
        attn_s[g] = attn_s[g] + weigh(g, 1)
        refill(k_copy, 2 * g + 2)
        refill(v_copy, 2 * g + 1)
        for when, work in at.items():

            @pl.when(g == when)
            def _():
                for stage, c in work:
                    stage(c)

        return carry

    k_copy(0).wait()
    score(0, 0)
    refill(k_copy, 0)
    lax.fori_loop(0, groups - 1, step, 0)
    second_half(groups - 1)
    v_copy(steps - 1).wait()
    attn_s[groups - 1] = attn_s[groups - 1] + weigh(groups - 1, 1)
    for stage, c in tail:
        stage(c)
    for c in range(nc):
        mine, _ = place(c)
        wait_pieces(c, 0, send1[c], True)
        wait_pieces(c, 2, send2[c], True)

        @pl.when(mine)
        def _():
            waits(c, 1, recv1[c].at[pl.ds(0, n - 1)]).wait_send()
            waits(c, 3, recv1[c].at[pl.ds(0, n - 1)]).wait_send()

        wait_pieces(c, 3, send1[c])


def solution(mesh):
    n = mesh.shape["tp"]

    def step(x, k_cache, v_cache, gain_a, wq, wo, gain_m, w_gate, w_up, w_down):
        batch, cache = k_cache.shape[:2]
        d, ff = x.shape[1], w_gate.shape[1]
        nc = len(CHUNKS)
        bf, f32 = jnp.bfloat16, jnp.float32
        sizes = [(len(o), r, d // len(o)) for o, (_, r) in zip(OWNERS, CHUNKS)]
        per_chunk = []
        for half in range(2):
            per_chunk += [pltpu.VMEM((k, r, w), f32) for k, r, w in sizes]
            per_chunk += [pltpu.VMEM((k, r, w), bf) for k, r, w in sizes]
            per_chunk += [pltpu.VMEM((n, r, w), bf) for _, r, w in sizes]
            per_chunk += [pltpu.VMEM((r, w) if half else (k, r, w), bf) for k, r, w in sizes]
        return pl.pallas_call(
            functools.partial(kernel, n),
            out_shape=pltpu.VMEM(x.shape, x.dtype),
            in_specs=[pl.BlockSpec(memory_space=pltpu.HBM)] * 11,
            out_specs=pl.BlockSpec(memory_space=pltpu.VMEM),
            scratch_shapes=[
                pltpu.VMEM(x.shape, bf),
                pltpu.VMEM((d // LANES, LANES), bf),
                pltpu.VMEM((d // LANES, LANES), bf),
                pltpu.VMEM((8, HEAD), f32),
                pltpu.VMEM(wq.shape, bf),
                pltpu.VMEM(wo.shape, bf),
                pltpu.VMEM(w_gate.shape, bf),
                pltpu.VMEM(w_up.shape, bf),
                pltpu.VMEM(w_down.shape, bf),
                pltpu.VMEM((DEPTH, HALF, cache, HEAD), bf),
                pltpu.VMEM((DEPTH, HALF, cache, HEAD), bf),
                pltpu.VMEM((batch // GROUP, GROUP, HEAD), f32),
                pltpu.VMEM((batch // GROUP, GROUP, HEAD), f32),
                pltpu.VMEM((2, GROUP, cache), bf),
                *per_chunk,
                pltpu.SemaphoreType.DMA((9,)),
                pltpu.SemaphoreType.DMA((DEPTH,)),
                pltpu.SemaphoreType.DMA((DEPTH,)),
                pltpu.SemaphoreType.DMA((4, nc)),
                pltpu.SemaphoreType.DMA((4, nc)),
            ],
            compiler_params=pltpu.CompilerParams(
                collective_id=0, has_side_effects=True, vmem_limit_bytes=56 * 1024 * 1024
            ),
        )(
            x,
            gain_a.reshape(d // LANES, LANES),
            gain_m.reshape(d // LANES, LANES),
            jnp.asarray(turns(cache - 1)),
            wq,
            wo,
            w_gate,
            w_up,
            w_down,
            k_cache.reshape(batch, cache, HEAD),
            v_cache.reshape(batch, cache, HEAD),
        )

    states, cache, columns, rows_of = P("dp", None), P("dp", None, "tp", None), P(None, "tp"), P("tp", None)
    return jax.shard_map(
        step,
        mesh=mesh,
        in_specs=(states, cache, cache, P(None), columns, rows_of, P(None), columns, columns, rows_of),
        out_specs=states,
        check_vma=False,
    )
```
